32 devices in a mesh: layer: 4 (over y, x), row: 2 (over core), col: 4 (over z).
Axes of the slice: x: 2, y: 2, z: 4, core: 2. Of those that a mesh axis runs over, the one named last changes fastest.
Arguments:
- hidden: bfloat16 [384, 2304], P(('layer', 'row')), may hold values from -60 to 60
- embedding: bfloat16 [16384, 2304], P(('row', 'col'), 'layer'), may hold values from -0.3 to 0.3
- teacher: bfloat16 [384, 16384], P('layer', ('row', 'col')), may hold values from -80 to 240
Outputs:
- grad_embedding: float32 [16384, 2304], P(('row', 'col'), 'layer')
- grad_hidden: float32 [384, 2304], P(('layer', 'row', 'col'))
The draws below stay inside these ranges and needn't reach their ends.
All inputs are finite; a program needn't handle non-finite values.
Results may differ from the reference program's by a relative error of at most 0.0041.
Values may be sent and summed in bfloat16 or wider, within the bound.
A program may use at most 192 MiB of HBM per device.

```python
import math
import jax
import jax.numpy as jnp
from jax import lax

D = 2304
LOSS_SCALE = 256
TOKENS = 384
VOCAB = 16384


def embed_row(base_key, index):
    row_key = jax.random.fold_in(base_key, index)
    values = jnp.clip(jax.random.normal(row_key, (D,), jnp.float32), -6.0, 6.0) * D ** (-0.5)
    factor = 1.0 + 0.1 * index.astype(jnp.float32) / VOCAB
    bound = 14.4 * D ** (-0.5)
    return jnp.clip(values * factor, -bound, bound)


def embed_table(key):
    base_key = jax.random.fold_in(key, 11)
    return jax.vmap(lambda index: embed_row(base_key, index))(jnp.arange(VOCAB, dtype=jnp.int32))


def draw_embedding(key, part):
    return embed_table(key).astype(jnp.bfloat16)


def draw_hidden(key, part):
    drawn = jnp.clip(jax.random.normal(jax.random.fold_in(key, 21), (TOKENS, D), jnp.float32), -6.0, 6.0) * 3.0
    bound = 2880.0 * D ** (-0.5)
    return jnp.clip(drawn, -bound, bound).astype(jnp.bfloat16)


def draw_teacher(key, part):
    noise = jnp.clip(jax.random.normal(jax.random.fold_in(key, 41), (TOKENS, VOCAB), jnp.float32), -6.0, 6.0)
    rising = jnp.log(3.0) * jnp.arange(VOCAB, dtype=jnp.float32)[None, :] / VOCAB
    values = noise * 3.0 + rising
    return values.astype(jnp.bfloat16)


def setup_inputs(seed: int = 0) -> dict:
    streams_of = jax.random.split(jax.random.key(seed), 4)
    hidden = draw_hidden(jax.random.fold_in(streams_of[3], 71), 0)
    embedding = draw_embedding(jax.random.fold_in(streams_of[3], 71), 0)
    teacher = draw_teacher(jax.random.fold_in(streams_of[3], 71), 0)
    return dict(hidden=hidden, embedding=embedding, teacher=teacher)


def reference(hidden, embedding, teacher):
    tokens = hidden.shape[0]
    block = math.gcd(tokens, 256)
    nblocks = tokens // block
    hid_blocks = hidden.reshape(nblocks, block, hidden.shape[1])
    tea_blocks = teacher.reshape(nblocks, block, teacher.shape[1])

    def one_block(acc_embed, pair):
        hid_part, tea_part = pair
        logits = lax.dot_general(hid_part, embedding, (((1,), (1,)), ((), ())), preferred_element_type=jnp.float32)
        teach_f = tea_part.astype(jnp.float32)
        top_s = jnp.max(logits, axis=1)
        top_t = jnp.max(teach_f, axis=1)
        sum_s = jnp.sum(jnp.exp(logits - top_s[:, None]), axis=1)
        sum_t = jnp.sum(jnp.exp(teach_f - top_t[:, None]), axis=1)
        lse_s = top_s + jnp.log(sum_s)
        lse_t = top_t + jnp.log(sum_t)
        prob_s = jnp.exp(logits - lse_s[:, None])
        prob_t = jnp.exp(teach_f - lse_t[:, None])
        grads = ((prob_s - prob_t) * LOSS_SCALE).astype(jnp.bfloat16)
        grad_hid = jnp.dot(grads, embedding, preferred_element_type=jnp.float32)
        acc_embed = acc_embed + lax.dot_general(grads, hid_part, (((0,), (0,)), ((), ())), preferred_element_type=jnp.float32)
        return acc_embed, grad_hid

    start_acc = jnp.zeros(embedding.shape, jnp.float32)
    grad_embedding, grad_hid = lax.scan(one_block, start_acc, (hid_blocks, tea_blocks))
    return grad_embedding, grad_hid.reshape(tokens, hidden.shape[1])
```

```python
import functools

import jax
import jax.numpy as jnp
from jax import lax
from jax.experimental import pallas as pl
from jax.experimental.pallas import tpu as pltpu
from jax.sharding import PartitionSpec as P

LOSS_SCALE = 256
LAYERS = 4
LANES = 128
MESH = pl.DeviceIdType.MESH
F32 = jnp.float32
BF16 = jnp.bfloat16


def kernel(nr, nc, h_ref, e_ref, t_ref, g_ref, wp_ref, gh_ref,
           hs, part, rx, ry, st_send, st_recv, hsend, hrecv, fsend,
           hid_s, hid_r, x_s, x_r, y_s, y_r, st_s, st_r, gx_s, gx_r, gy_s, gy_r,
           pc_s, pc_r, fin_s, fin_r):
    nl = LAYERS
    nrc = nr * nc
    rows, width = h_ref.shape[0], e_ref.shape[1]
    vocab = e_ref.shape[0]
    half = vocab // 2
    tok = t_ref.shape[0]
    q = tok // nrc
    l, r, c = lax.axis_index("layer"), lax.axis_index("row"), lax.axis_index("col")
    lx = l + 1 - 2 * (l % 2)
    ly = l + 2 - 4 * (l // 2)
    ld = 3 - l
    block = (l, lx, ly, ld)
    me = r * nc + c

    def remote(src, dst, ss, rs, dev):
        return pltpu.make_async_remote_copy(
            src_ref=src, dst_ref=dst, send_sem=ss, recv_sem=rs, device_id=dev, device_id_type=MESH)

    barrier = pltpu.get_barrier_semaphore()
    for d in range(nl):
        for jr in range(nr):
            if d or jr:
                pl.semaphore_signal(barrier, inc=1, device_id=(block[d], (r + jr) % nr, c), device_id_type=MESH)
    for jr in range(nr):
        for jc in range(1, nc):
            pl.semaphore_signal(barrier, inc=1, device_id=(l, (r + jr) % nr, (c + jc) % nc), device_id_type=MESH)

    for i in range(nl):
        hs[i] = h_ref[:, i * width:(i + 1) * width]
    wp_ref[l, r] = hs[l]
    pl.semaphore_wait(barrier, nl * nr - 1 + nr * (nc - 1))

    sends = []
    for d in (3, 1, 2, 0):
        for jr in range(nr):
            if d or jr:
                cp = remote(hs.at[block[d]], wp_ref.at[l, r], hid_s.at[d, jr], hid_r.at[d, jr],
                            (block[d], (r + jr) % nr, c))
                cp.start()
                sends.append(cp)

    def hidden_wait(d):
        for jr in range(nr):
            if d or jr:
                slot = wp_ref.at[block[d], (r + nr - jr) % nr]
                remote(slot, slot, hid_s.at[d, jr], hid_r.at[d, jr], (block[d], (r + jr) % nr, c)).wait_recv()

    def score(d, k):
        lhs = wp_ref[block[d]].reshape(nr * rows, width)
        part[d, k] = lax.dot_general(lhs, e_ref[k * half:(k + 1) * half, :], (((1,), (1,)), ((), ())),
                                     preferred_element_type=F32)

    def to_x(src, i):
        return remote(src, rx.at[i], x_s.at[i], x_r.at[i], (lx, r, c))

    def to_y(src, i):
        return remote(src, ry.at[i], y_s.at[i], y_r.at[i], (ly, r, c))

    hidden_wait(3)
    score(3, 0)
    x0 = to_x(part.at[3, 0], 0)
    x0.start()
    score(3, 1)
    y0 = to_y(part.at[3, 1], 0)
    y0.start()
    hidden_wait(1)
    score(1, 0)
    x1 = to_x(part.at[1, 0], 1)
    x1.start()
    hidden_wait(2)
    score(2, 1)
    y1 = to_y(part.at[2, 1], 1)
    y1.start()
    score(1, 1)
    score(2, 0)
    hidden_wait(0)
    score(0, 0)
    score(0, 1)

    teach = t_ref[...].astype(F32)
    top_t = jnp.max(teach, axis=1, keepdims=True)
    sum_t = jnp.sum(jnp.exp(teach - top_t), axis=1, keepdims=True)

    y0.wait_recv()
    part[1, 1] = part[1, 1] + ry[0]
    x2 = to_x(part.at[1, 1], 2)
    x2.start()
    x0.wait_recv()
    part[2, 0] = part[2, 0] + rx[0]
    y2 = to_y(part.at[2, 0], 2)
    y2.start()

    x1.wait_recv()
    part[0, 0] = part[0, 0] + rx[1]
    y1.wait_recv()
    part[0, 1] = part[0, 1] + ry[1]
    x2.wait_recv()
    part[0, 1] = part[0, 1] + rx[2]
    y2.wait_recv()
    part[0, 0] = part[0, 0] + ry[2]

    top_s = jnp.maximum(jnp.max(part[0, 0], axis=1, keepdims=True), jnp.max(part[0, 1], axis=1, keepdims=True))
    sum_s = (jnp.sum(jnp.exp(part[0, 0] - top_s), axis=1, keepdims=True)
             + jnp.sum(jnp.exp(part[0, 1] - top_s), axis=1, keepdims=True))
    tp = st_send.shape[1]
    lane = lax.broadcasted_iota(jnp.int32, (tok, LANES), 1)
    pack = jnp.where(lane == 0, top_s, jnp.where(lane == 1, sum_s, jnp.where(lane == 2, top_t, sum_t)))
    if tp > tok:
        pack = jnp.concatenate([pack, jnp.zeros((tp - tok, LANES), F32)], axis=0)
    st_send[...] = jnp.transpose(pack)[:8, :]
    st_recv[0] = st_send[...]

    def peer(j):
        k = (me + j) % nrc
        return (l, k // nc, k % nc)

    def stat_copy(j):
        return remote(st_send, st_recv.at[j], st_s.at[j], st_r.at[j], peer(j))

    @pl.loop(1, nrc)
    def _(j):
        stat_copy(j).start()

    @pl.loop(1, nrc)
    def _(j):
        stat_copy(j).wait_recv()

    tops = jnp.max(st_recv[...], axis=0)
    row_s = jnp.zeros((1, tp), F32)
    row_t = jnp.zeros((1, tp), F32)
    for j in range(nrc):
        row_s = row_s + st_recv[j, 1:2, :] * jnp.exp(st_recv[j, 0:1, :] - tops[0:1, :])
        row_t = row_t + st_recv[j, 3:4, :] * jnp.exp(st_recv[j, 2:3, :] - tops[2:3, :])
    lse_s = tops[0:1, :] + jnp.log(row_s)
    lse_t = tops[2:3, :] + jnp.log(row_t)
    sub = lax.broadcasted_iota(jnp.int32, (LANES, tp), 0)
    cols = jnp.transpose(jnp.where(sub == 0, lse_s, lse_t))
    lse_s = cols[:tok, 0:1]
    lse_t = cols[:tok, 1:2]

    def half_of(b, k):
        return g_ref.at[b, :, k * half:(k + 1) * half]

    def grad_x(b, k, i):
        return remote(half_of(b, k), half_of(b, k), gx_s.at[i], gx_r.at[i], (lx, r, c))

    def grad_y(b, k, i):
        return remote(half_of(b, k), half_of(b, k), gy_s.at[i], gy_r.at[i], (ly, r, c))

    for k in range(2):
        prob_s = jnp.exp(part[0, k] - lse_s)
        prob_t = jnp.exp(t_ref[:, k * half:(k + 1) * half].astype(F32) - lse_t)
        g_ref[l, :, k * half:(k + 1) * half] = ((prob_s - prob_t) * LOSS_SCALE).astype(BF16)
        if k == 0:
            sends.append(grad_x(l, 0, 0))
            sends[-1].start()
    for cp in (grad_y(l, 1, 0), grad_x(l, 1, 1), grad_y(l, 0, 1)):
        cp.start()
        sends.append(cp)

    def piece_copy(d, j):
        k = (me + j) % nrc
        return remote(hsend.at[d, k], hrecv.at[d, j], pc_s.at[d, j], pc_r.at[d, j], peer(j))

    def back(d):
        hp = jnp.dot(g_ref[block[d]], e_ref[...], preferred_element_type=F32)
        for k in range(nrc):
            hsend[d, k] = hp[k * q:(k + 1) * q, :]

        @pl.loop(1, nrc)
        def _(j):
            piece_copy(d, j).start()

    def finish(d):
        @pl.loop(1, nrc)
        def _(j):
            piece_copy(d, j).wait_recv()

        acc = hsend[d, me]
        for j in range(1, nrc):
            acc = acc + hrecv[d, j]
        if d == 0:
            gh_ref[l] = acc
        else:
            fsend[d] = acc
            cp = remote(fsend.at[d], gh_ref.at[l], fin_s.at[d], fin_r.at[d], (block[d], r, c))
            cp.start()
            sends.append(cp)

    back(0)
    grad_x(lx, 0, 0).wait_recv()
    cp = grad_y(lx, 0, 2)
    cp.start()
    sends.append(cp)
    grad_y(ly, 1, 0).wait_recv()
    cp = grad_x(ly, 1, 2)
    cp.start()
    sends.append(cp)
    finish(0)
    grad_x(lx, 1, 1).wait_recv()
    back(1)
    grad_y(ly, 0, 1).wait_recv()
    back(2)
    finish(1)
    finish(2)
    grad_x(ld, 1, 2).wait_recv()
    grad_y(ld, 0, 2).wait_recv()
    back(3)
    finish(3)
    for d in range(1, nl):
        remote(fsend.at[d], gh_ref.at[block[d]], fin_s.at[d], fin_r.at[d], (block[d], r, c)).wait_recv()

    for cp in sends + [x0, x1, x2, y0, y1, y2]:
        cp.wait_send()

    @pl.loop(1, nrc)
    def _(j):
        stat_copy(j).wait_send()
        for d in range(nl):
            piece_copy(d, j).wait_send()


def fused(nr, nc, hidden, embedding, teacher):
    nl = LAYERS
    nrc = nr * nc
    rows = hidden.shape[0]
    vocab, width = embedding.shape
    tok = teacher.shape[0]
    q = tok // nrc
    tp = -(-tok // LANES) * LANES
    dma = pltpu.SemaphoreType.DMA
    vmem = pl.BlockSpec(memory_space=pltpu.VMEM)
    return pl.pallas_call(
        functools.partial(kernel, nr, nc),
        out_shape=(
            jax.ShapeDtypeStruct((nl, tok, vocab), BF16),
            jax.ShapeDtypeStruct((nl, nr, rows, width), BF16),
            jax.ShapeDtypeStruct((nl, q, width), F32),
        ),
        in_specs=[vmem] * 3,
        out_specs=(vmem, vmem, vmem),
        scratch_shapes=[
            pltpu.VMEM((nl, rows, width), BF16),
            pltpu.VMEM((nl, 2, tok, vocab // 2), F32),
            pltpu.VMEM((3, tok, vocab // 2), F32),
            pltpu.VMEM((3, tok, vocab // 2), F32),
            pltpu.VMEM((8, tp), F32),
            pltpu.VMEM((nrc, 8, tp), F32),
            pltpu.VMEM((nl, nrc, q, width), F32),
            pltpu.VMEM((nl, nrc, q, width), F32),
            pltpu.VMEM((nl, q, width), F32),
            dma((nl, nr)), dma((nl, nr)),
            dma((3,)), dma((3,)), dma((3,)), dma((3,)),
            dma((nrc,)), dma((nrc,)),
            dma((3,)), dma((3,)), dma((3,)), dma((3,)),
            dma((nl, nrc)), dma((nl, nrc)),
            dma((nl,)), dma((nl,)),
        ],
        compiler_params=pltpu.CompilerParams(
            collective_id=0, has_side_effects=True, vmem_limit_bytes=62 * 1024 * 1024),
    )(hidden, embedding, teacher)


def solution(mesh):
    nl, nr, nc = mesh.shape["layer"], mesh.shape["row"], mesh.shape["col"]
    assert nl == LAYERS
    placed = (P(("layer", "row"), None), P(("row", "col"), "layer"), P("layer", ("row", "col")))

    def local(hidden, embedding, teacher):
        grads, width_part, pieces = fused(nr, nc, hidden, embedding, teacher)
        tokens = nl * teacher.shape[0]
        grad_embedding = lax.dot_general(
            grads.reshape(tokens, -1), width_part.reshape(tokens, -1),
            (((0,), (0,)), ((), ())), preferred_element_type=F32)
        grad_hidden = pieces.transpose(1, 0, 2).reshape(pieces.shape[1], -1)
        return grad_embedding, grad_hidden

    return jax.shard_map(
        local,
        mesh=mesh,
        in_specs=placed,
        out_specs=(P(("row", "col"), "layer"), P(("layer", "row", "col"), None)),
        check_vma=False,
    )
```

```python
import functools

import jax
import jax.numpy as jnp
from jax import lax
from jax.experimental import pallas as pl
from jax.experimental.pallas import tpu as pltpu
from jax.sharding import PartitionSpec as P

LOSS_SCALE = 256
LAYERS = 4
LANES = 128
MESH = pl.DeviceIdType.MESH
F32 = jnp.float32
BF16 = jnp.bfloat16


def kernel(nr, nc, h_in, e_in, t_in, g_out, wp_out, gh_ref,
           h_ref, e_ref, t_ref, g_ref, wp_ref, ghs,
           hs, part, rx, ry, st_send, st_recv, hsend, row_in, mid_sum, col_in, fsend,
           in_sem, out_sem, hid_s, hid_r, x_s, x_r, y_s, y_r, st_s, st_r, gx_s, gx_r, gy_s, gy_r,
           row_s, row_r, col_s, col_r, fin_s, fin_r):
    nl = LAYERS
    nrc = nr * nc
    rows = h_ref.shape[0]
    width, vocab = e_ref.shape
    half = vocab // 2
    tok = t_ref.shape[0]
    q = tok // nrc
    l, r, c = lax.axis_index("layer"), lax.axis_index("row"), lax.axis_index("col")
    lx = l + 1 - 2 * (l % 2)
    ly = l + 2 - 4 * (l // 2)
    ld = 3 - l
    block = (l, lx, ly, ld)
    me = r * nc + c

    def remote(src, dst, ss, rs, dev):
        return pltpu.make_async_remote_copy(
            src_ref=src, dst_ref=dst, send_sem=ss, recv_sem=rs, device_id=dev, device_id_type=MESH)

    loads = [pltpu.make_async_copy(src, dst, in_sem.at[i])
             for i, (src, dst) in enumerate(((h_in, h_ref), (e_in, e_ref), (t_in, t_ref)))]
    for cp in loads:
        cp.start()
    stores = []

    def store(src, dst):
        cp = pltpu.make_async_copy(src, dst, out_sem.at[len(stores)])
        cp.start()
        stores.append(cp)

    barrier = pltpu.get_barrier_semaphore()
    for d in range(nl):
        for jr in range(nr):
            if d or jr:
                pl.semaphore_signal(barrier, inc=1, device_id=(block[d], (r + jr) % nr, c), device_id_type=MESH)
    for jr in range(nr):
        for jc in range(1, nc):
            pl.semaphore_signal(barrier, inc=1, device_id=(l, (r + jr) % nr, (c + jc) % nc), device_id_type=MESH)

    loads[0].wait()
    for i in range(nl):
        hs[i] = h_ref[:, i * width:(i + 1) * width]
    wp_ref[l, r] = hs[l]
    pl.semaphore_wait(barrier, nl * nr - 1 + nr * (nc - 1))

    sends = []
    for d in (3, 1, 2):
        sends.append(remote(hs.at[block[d]], wp_ref.at[l, r], hid_s.at[d, 0], hid_r.at[d, 0], (block[d], r, c)))
        sends[-1].start()

    def hand_on(d):
        slot = wp_ref.at[block[d], r]
        if d:
            remote(slot, slot, hid_s.at[d, 0], hid_r.at[d, 0], (block[d], r, c)).wait_recv()
        for jr in range(1, nr):
            src = slot if d else hs.at[l]
            sends.append(remote(src, slot, hid_s.at[d, jr], hid_r.at[d, jr], (l, (r + jr) % nr, c)))
            sends[-1].start()

    def hidden_wait(d):
        for jr in range(1, nr):
            slot = wp_ref.at[block[d], (r + nr - jr) % nr]
            remote(slot, slot, hid_s.at[d, jr], hid_r.at[d, jr], (l, (r + jr) % nr, c)).wait_recv()

    def score(d, k):
        lhs = wp_ref[block[d]].reshape(nr * rows, width)
        part[d, k] = jnp.dot(lhs, e_ref[:, k * half:(k + 1) * half], preferred_element_type=F32)

    def to_x(src, i):
        return remote(src, rx.at[i], x_s.at[i], x_r.at[i], (lx, r, c))

    def to_y(src, i):
        return remote(src, ry.at[i], y_s.at[i], y_r.at[i], (ly, r, c))

    for d in (0, 3, 1, 2):
        hand_on(d)
    loads[1].wait()
    hidden_wait(3)
    score(3, 0)
    x0 = to_x(part.at[3, 0], 0)
    x0.start()
    score(3, 1)
    y0 = to_y(part.at[3, 1], 0)
    y0.start()
    hidden_wait(1)
    score(1, 0)
    x1 = to_x(part.at[1, 0], 1)
    x1.start()
    hidden_wait(2)
    score(2, 1)
    y1 = to_y(part.at[2, 1], 1)
    y1.start()
    score(1, 1)
    score(2, 0)
    hidden_wait(0)
    score(0, 0)
    score(0, 1)

    store(wp_ref, wp_out)
    loads[2].wait()
    teach = t_ref[...].astype(F32)
    top_t = jnp.max(teach, axis=1, keepdims=True)
    sum_t = jnp.sum(jnp.exp(teach - top_t), axis=1, keepdims=True)

    y0.wait_recv()
    part[1, 1] = part[1, 1] + ry[0]
    x2 = to_x(part.at[1, 1], 2)
    x2.start()
    x0.wait_recv()
    part[2, 0] = part[2, 0] + rx[0]
    y2 = to_y(part.at[2, 0], 2)
    y2.start()

    x1.wait_recv()
    part[0, 0] = part[0, 0] + rx[1]
    y1.wait_recv()
    part[0, 1] = part[0, 1] + ry[1]
    x2.wait_recv()
    part[0, 1] = part[0, 1] + rx[2]
    y2.wait_recv()
    part[0, 0] = part[0, 0] + ry[2]

    top_s = jnp.maximum(jnp.max(part[0, 0], axis=1, keepdims=True), jnp.max(part[0, 1], axis=1, keepdims=True))
    sum_s = (jnp.sum(jnp.exp(part[0, 0] - top_s), axis=1, keepdims=True)
             + jnp.sum(jnp.exp(part[0, 1] - top_s), axis=1, keepdims=True))
    tp = st_send.shape[1]
    lane = lax.broadcasted_iota(jnp.int32, (tok, LANES), 1)
    pack = jnp.where(lane == 0, top_s, jnp.where(lane == 1, sum_s, jnp.where(lane == 2, top_t, sum_t)))
    if tp > tok:
        pack = jnp.concatenate([pack, jnp.zeros((tp - tok, LANES), F32)], axis=0)
    st_send[...] = jnp.transpose(pack)[:8, :]
    st_recv[0] = st_send[...]

    def peer(j):
        k = (me + j) % nrc
        return (l, k // nc, k % nc)

    def stat_copy(j):
        return remote(st_send, st_recv.at[j], st_s.at[j], st_r.at[j], peer(j))

    @pl.loop(1, nrc)
    def _(j):
        stat_copy(j).start()

    @pl.loop(1, nrc)
    def _(j):
        stat_copy(j).wait_recv()

    tops = jnp.max(st_recv[...], axis=0)
    tot_s = jnp.zeros((1, tp), F32)
    tot_t = jnp.zeros((1, tp), F32)
    for j in range(nrc):
        tot_s = tot_s + st_recv[j, 1:2, :] * jnp.exp(st_recv[j, 0:1, :] - tops[0:1, :])
        tot_t = tot_t + st_recv[j, 3:4, :] * jnp.exp(st_recv[j, 2:3, :] - tops[2:3, :])
    lse_s = tops[0:1, :] + jnp.log(tot_s)
    lse_t = tops[2:3, :] + jnp.log(tot_t)
    sub = lax.broadcasted_iota(jnp.int32, (LANES, tp), 0)
    cols = jnp.transpose(jnp.where(sub == 0, lse_s, lse_t))
    lse_s = cols[:tok, 0:1]
    lse_t = cols[:tok, 1:2]

    def half_of(b, k):
        return g_ref.at[b, :, k * half:(k + 1) * half]

    def grad_x(b, k, i):
        return remote(half_of(b, k), half_of(b, k), gx_s.at[i], gx_r.at[i], (lx, r, c))

    def grad_y(b, k, i):
        return remote(half_of(b, k), half_of(b, k), gy_s.at[i], gy_r.at[i], (ly, r, c))

    for k in range(2):
        prob_s = jnp.exp(part[0, k] - lse_s)
        prob_t = jnp.exp(t_ref[:, k * half:(k + 1) * half].astype(F32) - lse_t)
        g_ref[l, :, k * half:(k + 1) * half] = ((prob_s - prob_t) * LOSS_SCALE).astype(BF16)
        if k == 0:
            sends.append(grad_x(l, 0, 0))
            sends[-1].start()
    for cp in (grad_y(l, 1, 0), grad_x(l, 1, 1), grad_y(l, 0, 1)):
        cp.start()
        sends.append(cp)

    def row_copy(d, j):
        to = (r + j) % nr
        return remote(hsend.at[d, to], row_in.at[d, j], row_s.at[d, j], row_r.at[d, j], (l, to, c))

    def col_copy(d, j):
        to = (c + j) % nc
        return remote(mid_sum.at[d, to], col_in.at[d, j], col_s.at[d, j], col_r.at[d, j], (l, r, to))

    def back(d):
        store(g_ref.at[block[d]], g_out.at[block[d]])
        hp = lax.dot_general(g_ref[block[d]], e_ref[...], (((1,), (1,)), ((), ())), preferred_element_type=F32)
        for i in range(nr):
            for k in range(nc):
                at = (i * nc + k) * q
                hsend[d, i, k] = hp[at:at + q, :]
        for j in range(1, nr):
            row_copy(d, j).start()

    def middle(d):
        for j in range(1, nr):
            row_copy(d, j).wait_recv()
        acc = hsend[d, r]
        for j in range(1, nr):
            acc = acc + row_in[d, j]
        mid_sum[d] = acc
        for j in range(1, nc):
            col_copy(d, j).start()

    def finish(d):
        for j in range(1, nc):
            col_copy(d, j).wait_recv()
        acc = mid_sum[d, c]
        for j in range(1, nc):
            acc = acc + col_in[d, j]
        if d == 0:
            ghs[l] = acc
        else:
            fsend[d] = acc
            cp = remote(fsend.at[d], ghs.at[l], fin_s.at[d], fin_r.at[d], (block[d], r, c))
            cp.start()
            sends.append(cp)

    back(0)
    middle(0)
    grad_x(lx, 0, 0).wait_recv()
    cp = grad_y(lx, 0, 2)
    cp.start()
    sends.append(cp)
    grad_y(ly, 1, 0).wait_recv()
    cp = grad_x(ly, 1, 2)
    cp.start()
    sends.append(cp)
    finish(0)
    grad_x(lx, 1, 1).wait_recv()
    back(1)
    grad_y(ly, 0, 1).wait_recv()
    back(2)
    middle(1)
    middle(2)
    finish(1)
    finish(2)
    grad_x(ld, 1, 2).wait_recv()
    grad_y(ld, 0, 2).wait_recv()
    back(3)
    middle(3)
    finish(3)
    for d in range(1, nl):
        remote(fsend.at[d], ghs.at[block[d]], fin_s.at[d], fin_r.at[d], (block[d], r, c)).wait_recv()
    for i in range(nl):
        gh_ref[:, i * width:(i + 1) * width] = ghs[i]

    for cp in sends + [x0, x1, x2, y0, y1, y2]:
        cp.wait_send()

    @pl.loop(1, nrc)
    def _(j):
        stat_copy(j).wait_send()

    for d in range(nl):
        for j in range(1, nr):
            row_copy(d, j).wait_send()
        for j in range(1, nc):
            col_copy(d, j).wait_send()
    for cp in stores:
        cp.wait()


def fused(nr, nc, hidden, embedding, teacher):
    nl = LAYERS
    nrc = nr * nc
    rows = hidden.shape[0]
    width, vocab = embedding.shape
    tok = teacher.shape[0]
    q = tok // nrc
    tp = -(-tok // LANES) * LANES
    dma = pltpu.SemaphoreType.DMA
    vmem = pl.BlockSpec(memory_space=pltpu.VMEM)
    hbm = pl.BlockSpec(memory_space=pl.ANY)
    return pl.pallas_call(
        functools.partial(kernel, nr, nc),
        out_shape=(
            jax.ShapeDtypeStruct((nl, tok, vocab), BF16),
            jax.ShapeDtypeStruct((nl, nr, rows, width), BF16),
            jax.ShapeDtypeStruct((q, nl * width), F32),
        ),
        in_specs=[hbm] * 3,
        out_specs=(hbm, hbm, vmem),
        scratch_shapes=[
            pltpu.VMEM((rows, nl * width), BF16),
            pltpu.VMEM((width, vocab), BF16),
            pltpu.VMEM((tok, vocab), BF16),
            pltpu.VMEM((nl, tok, vocab), BF16),
            pltpu.VMEM((nl, nr, rows, width), BF16),
            pltpu.VMEM((nl, q, width), F32),
            pltpu.VMEM((nl, rows, width), BF16),
            pltpu.VMEM((nl, 2, tok, vocab // 2), F32),
            pltpu.VMEM((3, tok, vocab // 2), F32),
            pltpu.VMEM((3, tok, vocab // 2), F32),
            pltpu.VMEM((8, tp), F32),
            pltpu.VMEM((nrc, 8, tp), F32),
            pltpu.VMEM((nl, nr, nc, q, width), F32),
            pltpu.VMEM((nl, nr, nc, q, width), F32),
            pltpu.VMEM((nl, nc, q, width), F32),
            pltpu.VMEM((nl, nc, q, width), F32),
            pltpu.VMEM((nl, q, width), F32),
            dma((3,)), dma((nl + 1,)),
            dma((nl, nr)), dma((nl, nr)),
            dma((3,)), dma((3,)), dma((3,)), dma((3,)),
            dma((nrc,)), dma((nrc,)),
            dma((3,)), dma((3,)), dma((3,)), dma((3,)),
            dma((nl, nr)), dma((nl, nr)), dma((nl, nc)), dma((nl, nc)),
            dma((nl,)), dma((nl,)),
        ],
        compiler_params=pltpu.CompilerParams(
            collective_id=0, has_side_effects=True, vmem_limit_bytes=62 * 1024 * 1024),
    )(hidden, embedding, teacher)


def solution(mesh):
    nl, nr, nc = mesh.shape["layer"], mesh.shape["row"], mesh.shape["col"]
    assert nl == LAYERS
    placed = (P(("layer", "row"), None), P(("row", "col"), "layer"), P("layer", ("row", "col")))

    def local(hidden, embedding, teacher):
        grads, width_part, grad_hidden = fused(nr, nc, hidden, embedding.T, teacher)
        tokens = nl * teacher.shape[0]
        grad_embedding = lax.dot_general(
            grads.reshape(tokens, -1), width_part.reshape(tokens, -1),
            (((0,), (0,)), ((), ())), preferred_element_type=F32)
        return grad_embedding, grad_hidden

    return jax.shard_map(
        local,
        mesh=mesh,
        in_specs=placed,
        out_specs=(P(("row", "col"), "layer"), P(("layer", "row", "col"), None)),
        check_vma=False,
    )
```

```python
import functools

import jax
import jax.numpy as jnp
from jax import lax
from jax.experimental import pallas as pl
from jax.experimental.pallas import tpu as pltpu
from jax.sharding import PartitionSpec as P

LOSS_SCALE = 256
LAYERS = 4
LANES = 128
MESH = pl.DeviceIdType.MESH
F32 = jnp.float32
BF16 = jnp.bfloat16


def kernel(nr, nc, h_in, e_in, t_in, ge_ref, gh_ref,
           h_ref, e_ref, et_ref, t_ref, g_ref, wp_ref, wpt_ref, ghs,
           hs, part, rx, ry, st_send, st_recv, hsend, row_in, mid_sum, col_in, fsend,
           in_sem, hid_s, hid_r, x_s, x_r, y_s, y_r, st_s, st_r, gx_s, gx_r, gy_s, gy_r,
           row_s, row_r, col_s, col_r, fin_s, fin_r):
    nl = LAYERS
    nrc = nr * nc
    rows = h_ref.shape[0]
    width, vocab = e_ref.shape
    half = vocab // 2
    tok = t_ref.shape[0]
    q = tok // nrc
    l, r, c = lax.axis_index("layer"), lax.axis_index("row"), lax.axis_index("col")
    lx = l + 1 - 2 * (l % 2)
    ly = l + 2 - 4 * (l // 2)
    ld = 3 - l
    block = (l, lx, ly, ld)
    me = r * nc + c

    def remote(src, dst, ss, rs, dev):
        return pltpu.make_async_remote_copy(
            src_ref=src, dst_ref=dst, send_sem=ss, recv_sem=rs, device_id=dev, device_id_type=MESH)

    loads = [pltpu.make_async_copy(src, dst, in_sem.at[i])
             for i, (src, dst) in enumerate(((h_in, h_ref), (e_in, e_ref), (t_in, t_ref)))]
    for cp in loads:
        cp.start()
    barrier = pltpu.get_barrier_semaphore()
    for d in range(nl):
        for jr in range(nr):
            if d or jr:
                pl.semaphore_signal(barrier, inc=1, device_id=(block[d], (r + jr) % nr, c), device_id_type=MESH)
    for jr in range(nr):
        for jc in range(1, nc):
            pl.semaphore_signal(barrier, inc=1, device_id=(l, (r + jr) % nr, (c + jc) % nc), device_id_type=MESH)

    loads[0].wait()
    for i in range(nl):
        hs[i] = h_ref[:, i * width:(i + 1) * width]
    wp_ref[l, r] = hs[l]
    pl.semaphore_wait(barrier, nl * nr - 1 + nr * (nc - 1))

    sends = []
    for d in (3, 1, 2):
        sends.append(remote(hs.at[block[d]], wp_ref.at[l, r], hid_s.at[d, 0], hid_r.at[d, 0], (block[d], r, c)))
        sends[-1].start()

    def hand_on(d):
        slot = wp_ref.at[block[d], r]
        if d:
            remote(slot, slot, hid_s.at[d, 0], hid_r.at[d, 0], (block[d], r, c)).wait_recv()
        for jr in range(1, nr):
            src = slot if d else hs.at[l]
            sends.append(remote(src, slot, hid_s.at[d, jr], hid_r.at[d, jr], (l, (r + jr) % nr, c)))
            sends[-1].start()

    def hidden_wait(d):
        for jr in range(1, nr):
            slot = wp_ref.at[block[d], (r + nr - jr) % nr]
            remote(slot, slot, hid_s.at[d, jr], hid_r.at[d, jr], (l, (r + jr) % nr, c)).wait_recv()

    def score(d, k):
        lhs = wp_ref[block[d]].reshape(nr * rows, width)
        part[d, k] = jnp.dot(lhs, e_ref[:, k * half:(k + 1) * half], preferred_element_type=F32)

    def to_x(src, i):
        return remote(src, rx.at[i], x_s.at[i], x_r.at[i], (lx, r, c))

    def to_y(src, i):
        return remote(src, ry.at[i], y_s.at[i], y_r.at[i], (ly, r, c))

    for d in (0, 3, 1, 2):
        hand_on(d)
    loads[1].wait()
    hidden_wait(3)
    score(3, 0)
    x0 = to_x(part.at[3, 0], 0)
    x0.start()
    score(3, 1)
    y0 = to_y(part.at[3, 1], 0)
    y0.start()
    hidden_wait(1)
    score(1, 0)
    x1 = to_x(part.at[1, 0], 1)
    x1.start()
    hidden_wait(2)
    score(2, 1)
    y1 = to_y(part.at[2, 1], 1)
    y1.start()
    score(1, 1)
    score(2, 0)
    hidden_wait(0)
    score(0, 0)
    score(0, 1)
    piece = width // nl if (width // nl) % 16 == 0 else width
    for i in range(0, width, piece):
        et_ref[:, i:i + piece] = jnp.transpose(e_ref[i:i + piece, :])
    wpt_ref[...] = jnp.transpose(wp_ref[...].reshape(nl * tok, width))

    loads[2].wait()
    teach = t_ref[...].astype(F32)
    top_t = jnp.max(teach, axis=1, keepdims=True)
    sum_t = jnp.sum(jnp.exp(teach - top_t), axis=1, keepdims=True)

    y0.wait_recv()
    part[1, 1] = part[1, 1] + ry[0]
    x2 = to_x(part.at[1, 1], 2)
    x2.start()
    x0.wait_recv()
    part[2, 0] = part[2, 0] + rx[0]
    y2 = to_y(part.at[2, 0], 2)
    y2.start()

    x1.wait_recv()
    part[0, 0] = part[0, 0] + rx[1]
    y1.wait_recv()
    part[0, 1] = part[0, 1] + ry[1]
    x2.wait_recv()
    part[0, 1] = part[0, 1] + rx[2]
    y2.wait_recv()
    part[0, 0] = part[0, 0] + ry[2]

    top_s = jnp.maximum(jnp.max(part[0, 0], axis=1, keepdims=True), jnp.max(part[0, 1], axis=1, keepdims=True))
    sum_s = (jnp.sum(jnp.exp(part[0, 0] - top_s), axis=1, keepdims=True)
             + jnp.sum(jnp.exp(part[0, 1] - top_s), axis=1, keepdims=True))
    tp = st_send.shape[1]
    lane = lax.broadcasted_iota(jnp.int32, (tok, LANES), 1)
    pack = jnp.where(lane == 0, top_s, jnp.where(lane == 1, sum_s, jnp.where(lane == 2, top_t, sum_t)))
    if tp > tok:
        pack = jnp.concatenate([pack, jnp.zeros((tp - tok, LANES), F32)], axis=0)
    st_send[...] = jnp.transpose(pack)[:8, :]
    st_recv[0] = st_send[...]

    def peer(j):
        k = (me + j) % nrc
        return (l, k // nc, k % nc)

    def stat_copy(j):
        return remote(st_send, st_recv.at[j], st_s.at[j], st_r.at[j], peer(j))

    @pl.loop(1, nrc)
    def _(j):
        stat_copy(j).start()

    @pl.loop(1, nrc)
    def _(j):
        stat_copy(j).wait_recv()

    tops = jnp.max(st_recv[...], axis=0)
    tot_s = jnp.zeros((1, tp), F32)
    tot_t = jnp.zeros((1, tp), F32)
    for j in range(nrc):
        tot_s = tot_s + st_recv[j, 1:2, :] * jnp.exp(st_recv[j, 0:1, :] - tops[0:1, :])
        tot_t = tot_t + st_recv[j, 3:4, :] * jnp.exp(st_recv[j, 2:3, :] - tops[2:3, :])
    lse_s = tops[0:1, :] + jnp.log(tot_s)
    lse_t = tops[2:3, :] + jnp.log(tot_t)
    sub = lax.broadcasted_iota(jnp.int32, (LANES, tp), 0)
    cols = jnp.transpose(jnp.where(sub == 0, lse_s, lse_t))
    lse_s = cols[:tok, 0:1]
    lse_t = cols[:tok, 1:2]

    def half_of(b, k):
        return g_ref.at[b, :, k * half:(k + 1) * half]

    def grad_x(b, k, i):
        return remote(half_of(b, k), half_of(b, k), gx_s.at[i], gx_r.at[i], (lx, r, c))

    def grad_y(b, k, i):
        return remote(half_of(b, k), half_of(b, k), gy_s.at[i], gy_r.at[i], (ly, r, c))

    for k in range(2):
        prob_s = jnp.exp(part[0, k] - lse_s)
        prob_t = jnp.exp(t_ref[:, k * half:(k + 1) * half].astype(F32) - lse_t)
        g_ref[l, :, k * half:(k + 1) * half] = ((prob_s - prob_t) * LOSS_SCALE).astype(BF16)
        if k == 0:
            sends.append(grad_x(l, 0, 0))
            sends[-1].start()
    for cp in (grad_y(l, 1, 0), grad_x(l, 1, 1), grad_y(l, 0, 1)):
        cp.start()
        sends.append(cp)

    def row_copy(d, j):
        to = (r + j) % nr
        return remote(hsend.at[d, to], row_in.at[d, j], row_s.at[d, j], row_r.at[d, j], (l, to, c))

    def col_copy(d, j):
        to = (c + j) % nc
        return remote(mid_sum.at[d, to], col_in.at[d, j], col_s.at[d, j], col_r.at[d, j], (l, r, to))

    def back(d):
        hp = jnp.dot(g_ref[block[d]], et_ref[...], preferred_element_type=F32)
        for i in range(nr):
            for k in range(nc):
                at = (i * nc + k) * q
                hsend[d, i, k] = hp[at:at + q, :]
        for j in range(1, nr):
            row_copy(d, j).start()

    def middle(d):
        for j in range(1, nr):
            row_copy(d, j).wait_recv()
        acc = hsend[d, r]
        for j in range(1, nr):
            acc = acc + row_in[d, j]
        mid_sum[d] = acc
        for j in range(1, nc):
            col_copy(d, j).start()

    def finish(d):
        for j in range(1, nc):
            col_copy(d, j).wait_recv()
        acc = mid_sum[d, c]
        for j in range(1, nc):
            acc = acc + col_in[d, j]
        if d == 0:
            ghs[l] = acc
        else:
            fsend[d] = acc
            cp = remote(fsend.at[d], ghs.at[l], fin_s.at[d], fin_r.at[d], (block[d], r, c))
            cp.start()
            sends.append(cp)

    def embed_part(lo, hi):
        for i in range(lo, hi):
            at = slice(i * vocab // 4, (i + 1) * vocab // 4)
            ge_ref[:, at] = jnp.dot(wpt_ref[...], g_ref[:, :, at].reshape(nl * tok, vocab // 4),
                                    preferred_element_type=F32)

    back(0)
    middle(0)
    grad_x(lx, 0, 0).wait_recv()
    cp = grad_y(lx, 0, 2)
    cp.start()
    sends.append(cp)
    grad_y(ly, 1, 0).wait_recv()
    cp = grad_x(ly, 1, 2)
    cp.start()
    sends.append(cp)
    finish(0)
    grad_x(lx, 1, 1).wait_recv()
    back(1)
    grad_y(ly, 0, 1).wait_recv()
    back(2)
    middle(1)
    middle(2)
    finish(1)
    finish(2)
    grad_x(ld, 1, 2).wait_recv()
    grad_y(ld, 0, 2).wait_recv()
    back(3)
    embed_part(0, 1)
    middle(3)
    embed_part(1, 4)
    finish(3)
    for d in range(1, nl):
        remote(fsend.at[d], ghs.at[block[d]], fin_s.at[d], fin_r.at[d], (block[d], r, c)).wait_recv()
    for i in range(nl):
        gh_ref[:, i * width:(i + 1) * width] = ghs[i]

    for cp in sends + [x0, x1, x2, y0, y1, y2]:
        cp.wait_send()

    @pl.loop(1, nrc)
    def _(j):
        stat_copy(j).wait_send()

    for d in range(nl):
        for j in range(1, nr):
            row_copy(d, j).wait_send()
        for j in range(1, nc):
            col_copy(d, j).wait_send()


def fused(nr, nc, hidden, embedding, teacher):
    nl = LAYERS
    nrc = nr * nc
    rows = hidden.shape[0]
    width, vocab = embedding.shape
    tok = teacher.shape[0]
    q = tok // nrc
    tp = -(-tok // LANES) * LANES
    dma = pltpu.SemaphoreType.DMA
    vmem = pl.BlockSpec(memory_space=pltpu.VMEM)
    hbm = pl.BlockSpec(memory_space=pl.ANY)
    return pl.pallas_call(
        functools.partial(kernel, nr, nc),
        out_shape=(
            pltpu.VMEM((width, vocab), F32),
            pltpu.VMEM((q, nl * width), F32),
        ),
        in_specs=[hbm] * 3,
        out_specs=(vmem, vmem),
        scratch_shapes=[
            pltpu.VMEM((rows, nl * width), BF16),
            pltpu.VMEM((width, vocab), BF16),
            pltpu.VMEM((vocab, width), BF16),
            pltpu.VMEM((tok, vocab), BF16),
            pltpu.VMEM((nl, tok, vocab), BF16),
            pltpu.VMEM((nl, nr, rows, width), BF16),
            pltpu.VMEM((width, nl * tok), BF16),
            pltpu.VMEM((nl, q, width), F32),
            pltpu.VMEM((nl, rows, width), BF16),
            pltpu.VMEM((nl, 2, tok, vocab // 2), F32),
            pltpu.VMEM((3, tok, vocab // 2), F32),
            pltpu.VMEM((3, tok, vocab // 2), F32),
            pltpu.VMEM((8, tp), F32),
            pltpu.VMEM((nrc, 8, tp), F32),
            pltpu.VMEM((nl, nr, nc, q, width), F32),
            pltpu.VMEM((nl, nr, nc, q, width), F32),
            pltpu.VMEM((nl, nc, q, width), F32),
            pltpu.VMEM((nl, nc, q, width), F32),
            pltpu.VMEM((nl, q, width), F32),
            dma((3,)),
            dma((nl, nr)), dma((nl, nr)),
            dma((3,)), dma((3,)), dma((3,)), dma((3,)),
            dma((nrc,)), dma((nrc,)),
            dma((3,)), dma((3,)), dma((3,)), dma((3,)),
            dma((nl, nr)), dma((nl, nr)), dma((nl, nc)), dma((nl, nc)),
            dma((nl,)), dma((nl,)),
        ],
        compiler_params=pltpu.CompilerParams(
            collective_id=0, has_side_effects=True, vmem_limit_bytes=56 * 1024 * 1024),
    )(hidden, embedding, teacher)


def solution(mesh):
    nl, nr, nc = mesh.shape["layer"], mesh.shape["row"], mesh.shape["col"]
    assert nl == LAYERS
    placed = (P(("layer", "row"), None), P(("row", "col"), "layer"), P("layer", ("row", "col")))

    def local(hidden, embedding, teacher):
        grad_embedding, grad_hidden = fused(nr, nc, hidden, embedding.T, teacher)
        return grad_embedding.T, grad_hidden

    return jax.shard_map(
        local,
        mesh=mesh,
        in_specs=placed,
        out_specs=(P(("row", "col"), "layer"), P(("layer", "row", "col"), None)),
        check_vma=False,
    )
```

```python
import functools

import jax
import jax.numpy as jnp
from jax import lax
from jax.experimental import pallas as pl
from jax.experimental.pallas import tpu as pltpu
from jax.sharding import PartitionSpec as P

LOSS_SCALE = 256
LAYERS = 4
LANES = 128
MESH = pl.DeviceIdType.MESH
F32 = jnp.float32
BF16 = jnp.bfloat16


def kernel(nr, nc, h_in, e_in, t_in, ge_ref, gh_ref,
           h_ref, e_ref, et_ref, t_ref, g_ref, wp_ref, wpt_ref, ghs,
           hs, part, rx, ry, st_send, st_recv, hsend, row_in, mid_sum, col_in, fsend,
           in_sem, hid_s, hid_r, x_s, x_r, y_s, y_r, st_s, st_r, gx_s, gx_r, gy_s, gy_r,
           row_s, row_r, col_s, col_r, fin_s, fin_r):
    nl = LAYERS
    nrc = nr * nc
    rows = h_ref.shape[0]
    width, vocab = e_ref.shape
    half = vocab // 2
    tok = t_ref.shape[0]
    q = tok // nrc
    l, r, c = lax.axis_index("layer"), lax.axis_index("row"), lax.axis_index("col")
    lx = l + 1 - 2 * (l % 2)
    ly = l + 2 - 4 * (l // 2)
    ld = 3 - l
    block = (l, lx, ly, ld)
    me = r * nc + c

    def remote(src, dst, ss, rs, dev):
        return pltpu.make_async_remote_copy(
            src_ref=src, dst_ref=dst, send_sem=ss, recv_sem=rs, device_id=dev, device_id_type=MESH)

    loads = [pltpu.make_async_copy(src, dst, in_sem.at[i])
             for i, (src, dst) in enumerate(((h_in, h_ref), (e_in, e_ref), (t_in, t_ref)))]
    for cp in loads:
        cp.start()
    barrier = pltpu.get_barrier_semaphore()
    for d in range(nl):
        for jr in range(nr):
            if d or jr:
                pl.semaphore_signal(barrier, inc=1, device_id=(block[d], (r + jr) % nr, c), device_id_type=MESH)
    for jr in range(nr):
        for jc in range(1, nc):
            pl.semaphore_signal(barrier, inc=1, device_id=(l, (r + jr) % nr, (c + jc) % nc), device_id_type=MESH)

    loads[0].wait()
    for i in range(nl):
        hs[i] = h_ref[:, i * width:(i + 1) * width]
    wp_ref[l, r] = hs[l]
    pl.semaphore_wait(barrier, nl * nr - 1 + nr * (nc - 1))

    sends = []
    for d in (3, 1, 2):
        sends.append(remote(hs.at[block[d]], wp_ref.at[l, r], hid_s.at[d, 0], hid_r.at[d, 0], (block[d], r, c)))
        sends[-1].start()

    def hand_on(d):
        slot = wp_ref.at[block[d], r]
        if d:
            remote(slot, slot, hid_s.at[d, 0], hid_r.at[d, 0], (block[d], r, c)).wait_recv()
        for jr in range(1, nr):
            src = slot if d else hs.at[l]
            sends.append(remote(src, slot, hid_s.at[d, jr], hid_r.at[d, jr], (l, (r + jr) % nr, c)))
            sends[-1].start()

    def hidden_wait(d):
        for jr in range(1, nr):
            slot = wp_ref.at[block[d], (r + nr - jr) % nr]
            remote(slot, slot, hid_s.at[d, jr], hid_r.at[d, jr], (l, (r + jr) % nr, c)).wait_recv()

    def score(d, k):
        lhs = wp_ref[block[d]].reshape(nr * rows, width)
        part[d, k] = jnp.dot(lhs, e_ref[:, k * half:(k + 1) * half], preferred_element_type=F32)

    def to_x(src, i):
        return remote(src, rx.at[i], x_s.at[i], x_r.at[i], (lx, r, c))

    def to_y(src, i):
        return remote(src, ry.at[i], y_s.at[i], y_r.at[i], (ly, r, c))

    for d in (0, 3, 1, 2):
        hand_on(d)
    loads[1].wait()
    hidden_wait(3)
    score(3, 0)
    x0 = to_x(part.at[3, 0], 0)
    x0.start()
    score(3, 1)
    y0 = to_y(part.at[3, 1], 0)
    y0.start()
    hidden_wait(1)
    score(1, 0)
    x1 = to_x(part.at[1, 0], 1)
    x1.start()
    hidden_wait(2)
    score(2, 1)
    y1 = to_y(part.at[2, 1], 1)
    y1.start()
    score(1, 1)
    score(2, 0)
    hidden_wait(0)
    score(0, 0)
    score(0, 1)
    piece = width // nl if (width // nl) % 16 == 0 else width
    for i in range(0, width, piece):
        et_ref[:, i:i + piece] = jnp.transpose(e_ref[i:i + piece, :])
    wpt_ref[...] = jnp.transpose(wp_ref[...].reshape(nl * tok, width))

    loads[2].wait()
    teach = t_ref[...].astype(F32)
    top_t = jnp.max(teach, axis=1, keepdims=True)
    sum_t = jnp.sum(jnp.exp(teach - top_t), axis=1, keepdims=True)

    y0.wait_recv()
    part[1, 1] = part[1, 1] + ry[0]
    x2 = to_x(part.at[1, 1], 2)
    x2.start()
    x0.wait_recv()
    part[2, 0] = part[2, 0] + rx[0]
    y2 = to_y(part.at[2, 0], 2)
    y2.start()

    x1.wait_recv()
    part[0, 0] = part[0, 0] + rx[1]
    y1.wait_recv()
    part[0, 1] = part[0, 1] + ry[1]
    x2.wait_recv()
    part[0, 1] = part[0, 1] + rx[2]
    y2.wait_recv()
    part[0, 0] = part[0, 0] + ry[2]

    top_s = jnp.maximum(jnp.max(part[0, 0], axis=1, keepdims=True), jnp.max(part[0, 1], axis=1, keepdims=True))
    sum_s = (jnp.sum(jnp.exp(part[0, 0] - top_s), axis=1, keepdims=True)
             + jnp.sum(jnp.exp(part[0, 1] - top_s), axis=1, keepdims=True))
    tp = st_send.shape[1]
    lane = lax.broadcasted_iota(jnp.int32, (tok, LANES), 1)
    pack = jnp.where(lane == 0, top_s, jnp.where(lane == 1, sum_s, jnp.where(lane == 2, top_t, sum_t)))
    if tp > tok:
        pack = jnp.concatenate([pack, jnp.zeros((tp - tok, LANES), F32)], axis=0)
    st_send[...] = jnp.transpose(pack)[:8, :]
    st_recv[0] = st_send[...]

    def peer(j):
        k = (me + j) % nrc
        return (l, k // nc, k % nc)

    def stat_copy(j):
        return remote(st_send, st_recv.at[j], st_s.at[j], st_r.at[j], peer(j))

    @pl.loop(1, nrc)
    def _(j):
        stat_copy(j).start()

    @pl.loop(1, nrc)
    def _(j):
        stat_copy(j).wait_recv()

    tops = jnp.max(st_recv[...], axis=0)
    tot_s = jnp.zeros((1, tp), F32)
    tot_t = jnp.zeros((1, tp), F32)
    for j in range(nrc):
        tot_s = tot_s + st_recv[j, 1:2, :] * jnp.exp(st_recv[j, 0:1, :] - tops[0:1, :])
        tot_t = tot_t + st_recv[j, 3:4, :] * jnp.exp(st_recv[j, 2:3, :] - tops[2:3, :])
    lse_s = tops[0:1, :] + jnp.log(tot_s)
    lse_t = tops[2:3, :] + jnp.log(tot_t)
    sub = lax.broadcasted_iota(jnp.int32, (LANES, tp), 0)
    cols = jnp.transpose(jnp.where(sub == 0, lse_s, lse_t))
    lse_s = cols[:tok, 0:1]
    lse_t = cols[:tok, 1:2]

    def half_of(b, k):
        return g_ref.at[b, :, k * half:(k + 1) * half]

    def grad_x(b, k, i):
        return remote(half_of(b, k), half_of(b, k), gx_s.at[i], gx_r.at[i], (lx, r, c))

    def grad_y(b, k, i):
        return remote(half_of(b, k), half_of(b, k), gy_s.at[i], gy_r.at[i], (ly, r, c))

    for k in range(2):
        prob_s = jnp.exp(part[0, k] - lse_s)
        prob_t = jnp.exp(t_ref[:, k * half:(k + 1) * half].astype(F32) - lse_t)
        g_ref[l, :, k * half:(k + 1) * half] = ((prob_s - prob_t) * LOSS_SCALE).astype(BF16)
        if k == 0:
            sends.append(grad_x(l, 0, 0))
            sends[-1].start()
    for cp in (grad_y(l, 1, 0), grad_x(l, 1, 1), grad_y(l, 0, 1)):
        cp.start()
        sends.append(cp)

    def row_copy(d, j):
        to = (r + j) % nr
        return remote(hsend.at[d, to], row_in.at[d, j], row_s.at[d, j], row_r.at[d, j], (l, to, c))

    def col_copy(d, j):
        to = (c + j) % nc
        return remote(mid_sum.at[d, to], col_in.at[d, j], col_s.at[d, j], col_r.at[d, j], (l, r, to))

    def back(d):
        hp = jnp.dot(g_ref[block[d]], et_ref[...], preferred_element_type=F32)
        for i in range(nr):
            for k in range(nc):
                at = (i * nc + k) * q
                hsend[d, i, k] = hp[at:at + q, :]
        for j in range(1, nr):
            row_copy(d, j).start()

    def middle(d):
        for j in range(1, nr):
            row_copy(d, j).wait_recv()
        acc = hsend[d, r]
        for j in range(1, nr):
            acc = acc + row_in[d, j]
        mid_sum[d] = acc
        for j in range(1, nc):
            col_copy(d, j).start()

    def finish(d):
        for j in range(1, nc):
            col_copy(d, j).wait_recv()
        acc = mid_sum[d, c]
        for j in range(1, nc):
            acc = acc + col_in[d, j]
        if d == 0:
            ghs[l] = acc
        else:
            fsend[d] = acc
            cp = remote(fsend.at[d], ghs.at[l], fin_s.at[d], fin_r.at[d], (block[d], r, c))
            cp.start()
            sends.append(cp)

    def embed_part(lo, hi):
        for i in range(lo, hi):
            at = slice(i * vocab // 4, (i + 1) * vocab // 4)
            ge_ref[:, at] = jnp.dot(wpt_ref[...], g_ref[:, :, at].reshape(nl * tok, vocab // 4),
                                    preferred_element_type=F32)

    back(0)
    middle(0)
    grad_x(lx, 0, 0).wait_recv()
    cp = grad_y(lx, 0, 2)
    cp.start()
    sends.append(cp)
    grad_y(ly, 1, 0).wait_recv()
    cp = grad_x(ly, 1, 2)
    cp.start()
    sends.append(cp)
    finish(0)
    grad_x(lx, 1, 1).wait_recv()
    back(1)
    grad_y(ly, 0, 1).wait_recv()
    back(2)
    middle(1)
    middle(2)
    grad_x(ld, 1, 2).wait_recv()
    grad_y(ld, 0, 2).wait_recv()
    back(3)
    embed_part(0, 1)
    middle(3)
    embed_part(1, 2)
    finish(1)
    finish(2)
    embed_part(2, 4)
    finish(3)
    for d in range(1, nl):
        remote(fsend.at[d], ghs.at[block[d]], fin_s.at[d], fin_r.at[d], (block[d], r, c)).wait_recv()
    for i in range(nl):
        gh_ref[:, i * width:(i + 1) * width] = ghs[i]

    for cp in sends + [x0, x1, x2, y0, y1, y2]:
        cp.wait_send()

    @pl.loop(1, nrc)
    def _(j):
        stat_copy(j).wait_send()

    for d in range(nl):
        for j in range(1, nr):
            row_copy(d, j).wait_send()
        for j in range(1, nc):
            col_copy(d, j).wait_send()


def fused(nr, nc, hidden, embedding, teacher):
    nl = LAYERS
    nrc = nr * nc
    rows = hidden.shape[0]
    width, vocab = embedding.shape
    tok = teacher.shape[0]
    q = tok // nrc
    tp = -(-tok // LANES) * LANES
    dma = pltpu.SemaphoreType.DMA
    vmem = pl.BlockSpec(memory_space=pltpu.VMEM)
    hbm = pl.BlockSpec(memory_space=pl.ANY)
    return pl.pallas_call(
        functools.partial(kernel, nr, nc),
        out_shape=(
            pltpu.VMEM((width, vocab), F32),
            pltpu.VMEM((q, nl * width), F32),
        ),
        in_specs=[hbm] * 3,
        out_specs=(vmem, vmem),
        scratch_shapes=[
            pltpu.VMEM((rows, nl * width), BF16),
            pltpu.VMEM((width, vocab), BF16),
            pltpu.VMEM((vocab, width), BF16),
            pltpu.VMEM((tok, vocab), BF16),
            pltpu.VMEM((nl, tok, vocab), BF16),
            pltpu.VMEM((nl, nr, rows, width), BF16),
            pltpu.VMEM((width, nl * tok), BF16),
            pltpu.VMEM((nl, q, width), F32),
            pltpu.VMEM((nl, rows, width), BF16),
            pltpu.VMEM((nl, 2, tok, vocab // 2), F32),
            pltpu.VMEM((3, tok, vocab // 2), F32),
            pltpu.VMEM((3, tok, vocab // 2), F32),
            pltpu.VMEM((8, tp), F32),
            pltpu.VMEM((nrc, 8, tp), F32),
            pltpu.VMEM((nl, nr, nc, q, width), F32),
            pltpu.VMEM((nl, nr, nc, q, width), F32),
            pltpu.VMEM((nl, nc, q, width), F32),
            pltpu.VMEM((nl, nc, q, width), F32),
            pltpu.VMEM((nl, q, width), F32),
            dma((3,)),
            dma((nl, nr)), dma((nl, nr)),
            dma((3,)), dma((3,)), dma((3,)), dma((3,)),
            dma((nrc,)), dma((nrc,)),
            dma((3,)), dma((3,)), dma((3,)), dma((3,)),
            dma((nl, nr)), dma((nl, nr)), dma((nl, nc)), dma((nl, nc)),
            dma((nl,)), dma((nl,)),
        ],
        compiler_params=pltpu.CompilerParams(
            collective_id=0, has_side_effects=True, vmem_limit_bytes=56 * 1024 * 1024),
    )(hidden, embedding, teacher)


def solution(mesh):
    nl, nr, nc = mesh.shape["layer"], mesh.shape["row"], mesh.shape["col"]
    assert nl == LAYERS
    placed = (P(("layer", "row"), None), P(("row", "col"), "layer"), P("layer", ("row", "col")))

    def local(hidden, embedding, teacher):
        grad_embedding, grad_hidden = fused(nr, nc, hidden, embedding.T, teacher)
        return grad_embedding.T, grad_hidden

    return jax.shard_map(
        local,
        mesh=mesh,
        in_specs=placed,
        out_specs=(P(("row", "col"), "layer"), P(("layer", "row", "col"), None)),
        check_vma=False,
    )
```
